512 devices in a mesh: groups: 2 (over y), row: 32 (over z), col: 4 (over x), rep: 2 (over core).
Axes of the slice: x: 4, y: 2, z: 32, core: 2. Of those that a mesh axis runs over, the one named last changes fastest.
The devices are a block of a 4x8x32 slice.
Arguments:
- kernel: float32 [32768, 16384], P(('groups', 'row'), ('col', 'rep')), parts along dimension 0, may hold values from 0 to 2, as said below
- source: float32 [64, 16384], P('groups', 'row'), parts along dimension 0, may hold values from 0.5 to 2, as said below
- target: float32 [64, 16384], P('groups', ('col', 'rep')), parts along dimension 0, may hold values from 0.5 to 2, as said below
Outputs:
- left_scale: float32 [64, 16384], P('groups', 'row'), parts along dimension 0
- right_scale: float32 [64, 16384], P('groups', ('col', 'rep')), parts along dimension 0
- errors: float32 [6, 32], P('groups'), parts along dimension 0
The draws below stay inside these ranges and needn't reach their ends.
There are 2 independent parts, one for each index of `groups`. The reference program is written for one: setup_inputs(seed, part) draws one part's arguments, and reference() takes and returns one part's arrays. A program takes and returns all parts, laid end to end along the dimension named above; each array names one. Nothing has to cross between parts.
Inputs may be any that keep to these rules, and one draw needn't show every extreme that they name: `kernel`: every entry is positive. `source`: every entry is positive. `target`: every entry is positive.
All inputs are finite; a program needn't handle non-finite values.
Results may differ from the reference program's by a relative error of at most 0.0001.
Values sent between devices are 32-bit elements; how exact they have to be, the bound alone decides.
No kernel may reach another device: no remote copies, remote signals or barrier semaphores. Data moves between devices by JAX's collectives and lax.ppermute only.
A program may use at most 64 MiB of HBM per device.

```python
import math
import jax
import jax.numpy as jnp
from jax import lax

N = 16384
PAIRS = 32
ITERS = 3


def support_points(key):
    folded = jax.random.fold_in(key, 31)
    point_key, sink_key = jax.random.split(folded)
    source_points = jax.random.uniform(point_key, (N, 3), jnp.float32)
    target_points = jax.random.uniform(sink_key, (N, 3), jnp.float32)
    return (source_points, target_points)


def draw_kernel(key, part):
    source_points, target_points = support_points(key)
    row_key, col_key = jax.random.split(jax.random.fold_in(key, 11))
    top = math.log(10.0)
    spread = 0.025
    rows_log = jax.random.uniform(row_key, (N, 1), jnp.float32, 0.0, top)
    cols_log = jax.random.uniform(col_key, (1, N), jnp.float32, 0.0, top)
    source_norms = jnp.sum(source_points * source_points, axis=1)
    target_norms = jnp.sum(target_points * target_points, axis=1)
    cross = jnp.dot(source_points, target_points.T, precision=lax.Precision.HIGHEST)
    squared = jnp.maximum(source_norms[:, None] + target_norms[None, :] - 2.0 * cross, 0.0)
    raw = jnp.exp(rows_log + cols_log) * (jnp.exp(-squared / spread) + 0.005)
    return raw * (N / jnp.sum(raw))


def marginal_draw(folded):
    values = jnp.exp(jax.random.uniform(folded, (PAIRS, N), jnp.float32, math.log(0.5), math.log(2.0)))
    return values


def draw_source(key, part):
    return marginal_draw(jax.random.fold_in(key, 41))


def draw_target(key, part):
    return marginal_draw(jax.random.fold_in(key, 23))


def setup_inputs(seed: int = 0, part: int = 0) -> dict:
    keys = jax.random.split(jax.random.key(seed), 4)
    part_keys = jax.random.split(jax.random.fold_in(keys[3], part), 4)
    return {
        "kernel": draw_kernel(jax.random.fold_in(jax.random.fold_in(keys[3], part), 71), part),
        "source": draw_source(jax.random.fold_in(jax.random.fold_in(keys[3], part), 71), part),
        "target": draw_target(jax.random.fold_in(jax.random.fold_in(keys[3], part), 71), part),
    }


def reference(kernel, source, target):
    right_scale = jnp.ones(target.shape, jnp.float32)
    errors = []
    left_scale = source
    for step in range(ITERS):
        kv = lax.dot_general(right_scale, kernel, (((1,), (1,)), ((), ())), precision=lax.Precision.HIGHEST)
        left_scale = source / kv
        ktu = jnp.dot(left_scale, kernel, precision=lax.Precision.HIGHEST)
        errors.append(jnp.sum(jnp.abs(right_scale * ktu - target), axis=1) / N)
        right_scale = target / ktu
    return left_scale, right_scale, jnp.stack(errors)
```

```python
import jax
import jax.numpy as jnp
from jax import lax
from jax.sharding import Mesh, PartitionSpec as P

ITERS = 3
NEAR = 4


def exchange(pieces, axis):
    return lax.all_to_all(pieces, axis, split_axis=0, concat_axis=0, tiled=True)


def from_everyone(array, axis, size):
    return exchange(jnp.broadcast_to(array, (size, *array.shape)), axis)


def solution(mesh):
    shape = mesh.shape
    far = shape["row"] // NEAR
    names = ("groups", "far", "near", "col", "rep")
    split = Mesh(
        mesh.devices.reshape(shape["groups"], far, NEAR, shape["col"], shape["rep"]), names
    )
    block = ("col", "rep")
    blocks = shape["col"] * shape["rep"]

    def total_over_rows(back):
        pairs, columns = back.shape
        few, share = pairs // NEAR, columns // far
        near = exchange(back.reshape(NEAR, few, columns), "near").sum(axis=0)
        pieces = near.reshape(few, far, share).transpose(1, 0, 2)
        piece = exchange(pieces, "far").sum(axis=0)
        mine = from_everyone(piece, "far", far)
        everything = from_everyone(mine, "near", NEAR)
        return everything.transpose(0, 2, 1, 3).reshape(pairs, columns)

    def local(kernel, source, target):
        count = blocks * target.shape[1]
        right_scale = jnp.ones(target.shape, jnp.float32)
        terms = []
        for step in range(ITERS):
            if step == 0:
                partial_value = jnp.sum(kernel, axis=1).reshape(-1, 128)
                value = from_everyone(partial_value, block, blocks).sum(axis=0).reshape(1, -1)
            else:
                partial_value = lax.dot_general(
                    right_scale, kernel, (((1,), (1,)), ((), ())), precision=lax.Precision.HIGH
                )
                value = from_everyone(partial_value, block, blocks).sum(axis=0)
            left_scale = source / value
            back = jnp.dot(left_scale, kernel, precision=lax.Precision.HIGH)
            total = total_over_rows(back)
            terms.append(jnp.sum(jnp.abs(right_scale * total - target), axis=1))
            right_scale = target / total
        errors = from_everyone(jnp.stack(terms), block, blocks).sum(axis=0) / count
        return left_scale, right_scale, errors

    return jax.shard_map(
        local,
        mesh=split,
        in_specs=(
            P(("groups", "far", "near"), block),
            P("groups", ("far", "near")),
            P("groups", block),
        ),
        out_specs=(P("groups", ("far", "near")), P("groups", block), P("groups", None)),
        check_vma=False,
    )
```

```python
import jax
import jax.numpy as jnp
from jax import lax
from jax.experimental import pallas as pl
from jax.experimental.pallas import tpu as pltpu
from jax.sharding import Mesh, PartitionSpec as P

ITERS = 3
NEAR = 8
SPLIT_STEPS = 4
LANES = 128
f32 = jnp.float32
bf16 = jnp.bfloat16
WHOLE = pl.BlockSpec(memory_space=pltpu.VMEM)
PARAMS = pltpu.CompilerParams(vmem_limit_bytes=8 * 2**20)
BY_LAST = (((1,), (1,)), ((), ()))


def halves(array):
    high = array.astype(bf16)
    return high, (array - high.astype(f32)).astype(bf16)


def cost(flops, *arrays):
    moved = sum(a.size * a.dtype.itemsize for a in arrays)
    return pl.CostEstimate(flops=flops, bytes_accessed=moved, transcendentals=0)


def split_body(kernel_ref, halves_ref, sums_ref):
    kernel = kernel_ref[...]
    halves_ref[0], halves_ref[1] = halves(kernel)
    part = kernel[:, :LANES]
    for start in range(LANES, kernel.shape[1], LANES):
        part = part + kernel[:, start : start + LANES]
    sums_ref[...] = jnp.sum(part.T, axis=0, keepdims=True)


def split(kernel):
    rows, columns = kernel.shape
    tile = rows // SPLIT_STEPS
    block = pl.BlockSpec((tile, columns), lambda i: (i, 0))
    return pl.pallas_call(
        split_body,
        grid=(SPLIT_STEPS,),
        in_specs=[block],
        out_specs=[
            pl.BlockSpec((2, tile, columns), lambda i: (0, i, 0)),
            pl.BlockSpec((1, tile), lambda i: (0, i)),
        ],
        out_shape=[
            jax.ShapeDtypeStruct((2, rows, columns), bf16),
            jax.ShapeDtypeStruct((1, rows), f32),
        ],
        compiler_params=PARAMS,
        cost_estimate=cost(4 * kernel.size, kernel, kernel),
        name="split",
    )(kernel)


def back_body(value_ref, source_ref, halves_ref, left_ref, back_ref):
    value = value_ref[0]
    for i in range(1, value_ref.shape[0]):
        value = value + value_ref[i]
    left = source_ref[...] / value
    left_ref[...] = left
    high, low = halves(left)
    both = jnp.concatenate([high, low], axis=0)
    pairs = left.shape[0]
    width = back_ref.shape[2]
    for m in range(back_ref.shape[0]):
        here = slice(m * width, (m + 1) * width)
        first = jnp.dot(both, halves_ref[0, :, here], preferred_element_type=f32)
        second = jnp.dot(high, halves_ref[1, :, here], preferred_element_type=f32)
        back_ref[m] = first[:pairs] + first[pairs:] + second


def scale_left(values, source, split_kernel):
    pairs, rows = source.shape
    columns = split_kernel.shape[2]
    pieces = jax.ShapeDtypeStruct((NEAR, pairs, columns // NEAR), f32)
    return pl.pallas_call(
        back_body,
        in_specs=[WHOLE] * 3,
        out_specs=[WHOLE] * 2,
        out_shape=[jax.ShapeDtypeStruct((pairs, rows), f32), pieces],
        compiler_params=PARAMS,
        cost_estimate=cost(3 * pairs * split_kernel.size, values, source, split_kernel, pieces),
        name="back",
    )(values, source, split_kernel)


def new_right(total_ref, target_ref, old_ref, right_ref, error_ref):
    pairs = target_ref.shape[0]
    width = total_ref.shape[2]
    error = jnp.zeros((pairs, width), f32)
    for m in range(total_ref.shape[0]):
        here = slice(m * width, (m + 1) * width)
        total = total_ref[m]
        target = target_ref[:, here]
        right_ref[:, here] = target / total
        error = error + jnp.abs(old_ref[:, here] * total - target)
    error_ref[...] = jnp.sum(error, axis=1, keepdims=True)


def value_body(total_ref, target_ref, old_ref, halves_ref, right_ref, error_ref, value_ref):
    new_right(total_ref, target_ref, old_ref, right_ref, error_ref)
    pairs = target_ref.shape[0]
    high, low = halves(right_ref[...])
    both = jnp.concatenate([high, low], axis=0)
    first = lax.dot_general(both, halves_ref[0], BY_LAST, preferred_element_type=f32)
    second = lax.dot_general(high, halves_ref[1], BY_LAST, preferred_element_type=f32)
    value = first[:pairs] + first[pairs:] + second
    for i in range(value_ref.shape[0]):
        value_ref[i] = value


def scale_right(totals, target, old, split_kernel=None, copies=1):
    pairs = target.shape[0]
    out = [jax.ShapeDtypeStruct(target.shape, f32), jax.ShapeDtypeStruct((pairs, 1), f32)]
    operands = [totals, target, old]
    flops = 4 * target.size
    if split_kernel is not None:
        operands += [split_kernel]
        out += [jax.ShapeDtypeStruct((copies, pairs, split_kernel.shape[1]), f32)]
        flops += 3 * pairs * split_kernel.size
    return pl.pallas_call(
        new_right if split_kernel is None else value_body,
        in_specs=[WHOLE] * len(operands),
        out_specs=[WHOLE] * len(out),
        out_shape=out,
        compiler_params=PARAMS,
        cost_estimate=cost(flops, *operands, *out),
        name="right" if split_kernel is None else "value",
    )(*operands)


def sum_body(pieces_ref, copies_ref):
    total = pieces_ref[0]
    for i in range(1, pieces_ref.shape[0]):
        total = total + pieces_ref[i]
    for i in range(copies_ref.shape[0]):
        copies_ref[i] = total


def summed(pieces, copies):
    out = jax.ShapeDtypeStruct((copies, *pieces.shape[1:]), f32)
    return pl.pallas_call(
        sum_body,
        in_specs=[WHOLE],
        out_specs=WHOLE,
        out_shape=out,
        compiler_params=PARAMS,
        cost_estimate=cost(pieces.size, pieces, out),
        name="sum",
    )(pieces)


def exchange(pieces, axis):
    return lax.all_to_all(pieces, axis, split_axis=0, concat_axis=0, tiled=True)


def from_everyone(array, axis, size):
    return exchange(jnp.broadcast_to(array, (size, *array.shape)), axis)


def solution(mesh):
    shape = mesh.shape
    far = shape["row"] // NEAR
    split_mesh = Mesh(
        mesh.devices.reshape(shape["groups"], far, NEAR, shape["col"], shape["rep"]),
        ("groups", "far", "near", "col", "rep"),
    )
    block = ("col", "rep")
    blocks = shape["col"] * shape["rep"]

    def total_over_rows(pieces):
        pieces = exchange(summed(exchange(pieces, "near"), far), "far")
        return exchange(summed(pieces, NEAR), "near")

    def local(kernel, source, target):
        split_kernel, sums = split(kernel)
        values = from_everyone(sums, block, blocks)
        right_scale = jnp.ones(target.shape, f32)
        terms = []
        for step in range(ITERS):
            left_scale, pieces = scale_left(values, source, split_kernel)
            totals = total_over_rows(pieces)
            if step < ITERS - 1:
                right_scale, term, values = scale_right(
                    totals, target, right_scale, split_kernel, blocks
                )
                values = exchange(values, block)
            else:
                right_scale, term = scale_right(totals, target, right_scale)
            terms.append(term.reshape(-1))
        count = blocks * target.shape[1]
        errors = from_everyone(jnp.stack(terms), block, blocks).sum(axis=0) / count
        return left_scale, right_scale, errors

    return jax.shard_map(
        local,
        mesh=split_mesh,
        in_specs=(
            P(("groups", "far", "near"), block),
            P("groups", ("far", "near")),
            P("groups", block),
        ),
        out_specs=(P("groups", ("far", "near")), P("groups", block), P("groups", None)),
        check_vma=False,
    )
```

```python
import jax
import jax.numpy as jnp
from jax import lax
from jax.experimental import pallas as pl
from jax.experimental.pallas import tpu as pltpu
from jax.sharding import PartitionSpec as P

ITERS = 3
NEAR = 8
SPLIT_STEPS = 4
LANES = 128
f32 = jnp.float32
bf16 = jnp.bfloat16
WHOLE = pl.BlockSpec(memory_space=pltpu.VMEM)
PARAMS = pltpu.CompilerParams(vmem_limit_bytes=8 * 2**20)
BY_LAST = (((1,), (1,)), ((), ()))


def halves(array):
    high = array.astype(bf16)
    return high, (array - high.astype(f32)).astype(bf16)


def cost(flops, *arrays):
    moved = sum(a.size * a.dtype.itemsize for a in arrays)
    return pl.CostEstimate(flops=flops, bytes_accessed=moved, transcendentals=0)


def split_body(kernel_ref, halves_ref, sums_ref):
    kernel = kernel_ref[...]
    halves_ref[0], halves_ref[1] = halves(kernel)
    part = kernel[:, :LANES]
    for start in range(LANES, kernel.shape[1], LANES):
        part = part + kernel[:, start : start + LANES]
    sums_ref[...] = jnp.sum(part.T, axis=0, keepdims=True)


def split(kernel):
    rows, columns = kernel.shape
    tile = rows // SPLIT_STEPS
    block = pl.BlockSpec((tile, columns), lambda i: (i, 0))
    return pl.pallas_call(
        split_body,
        grid=(SPLIT_STEPS,),
        in_specs=[block],
        out_specs=[
            pl.BlockSpec((2, tile, columns), lambda i: (0, i, 0)),
            pl.BlockSpec((1, tile), lambda i: (0, i)),
        ],
        out_shape=[
            jax.ShapeDtypeStruct((2, rows, columns), bf16),
            jax.ShapeDtypeStruct((1, rows), f32),
        ],
        compiler_params=PARAMS,
        cost_estimate=cost(4 * kernel.size, kernel, kernel),
        name="split",
    )(kernel)


def back_body(value_ref, source_ref, halves_ref, left_ref, back_ref):
    value = value_ref[0]
    for i in range(1, value_ref.shape[0]):
        value = value + value_ref[i]
    left = source_ref[...] / value
    left_ref[...] = left
    high, low = halves(left)
    both = jnp.concatenate([high, low], axis=0)
    pairs = left.shape[0]
    width = back_ref.shape[2]
    for m in range(back_ref.shape[0]):
        here = slice(m * width, (m + 1) * width)
        first = jnp.dot(both, halves_ref[0, :, here], preferred_element_type=f32)
        second = jnp.dot(high, halves_ref[1, :, here], preferred_element_type=f32)
        back_ref[m] = first[:pairs] + first[pairs:] + second


def scale_left(values, source, split_kernel):
    pairs, rows = source.shape
    columns = split_kernel.shape[2]
    pieces = jax.ShapeDtypeStruct((NEAR, pairs, columns // NEAR), f32)
    return pl.pallas_call(
        back_body,
        in_specs=[WHOLE] * 3,
        out_specs=[WHOLE] * 2,
        out_shape=[jax.ShapeDtypeStruct((pairs, rows), f32), pieces],
        compiler_params=PARAMS,
        cost_estimate=cost(3 * pairs * split_kernel.size, values, source, split_kernel, pieces),
        name="back",
    )(values, source, split_kernel)


def new_right(total_ref, target_ref, old_ref, right_ref, error_ref):
    pairs = target_ref.shape[0]
    width = total_ref.shape[2]
    error = jnp.zeros((pairs, width), f32)
    for m in range(total_ref.shape[0]):
        here = slice(m * width, (m + 1) * width)
        total = total_ref[m]
        target = target_ref[:, here]
        right_ref[:, here] = target / total
        error = error + jnp.abs(old_ref[:, here] * total - target)
    error_ref[...] = jnp.sum(error, axis=1, keepdims=True)


def value_body(total_ref, target_ref, old_ref, halves_ref, right_ref, error_ref, value_ref):
    new_right(total_ref, target_ref, old_ref, right_ref, error_ref)
    pairs = target_ref.shape[0]
    high, low = halves(right_ref[...])
    both = jnp.concatenate([high, low], axis=0)
    first = lax.dot_general(both, halves_ref[0], BY_LAST, preferred_element_type=f32)
    second = lax.dot_general(high, halves_ref[1], BY_LAST, preferred_element_type=f32)
    value = first[:pairs] + first[pairs:] + second
    for i in range(value_ref.shape[0]):
        value_ref[i] = value


def scale_right(totals, target, old, split_kernel=None, copies=1):
    pairs = target.shape[0]
    out = [jax.ShapeDtypeStruct(target.shape, f32), jax.ShapeDtypeStruct((pairs, 1), f32)]
    operands = [totals, target, old]
    flops = 4 * target.size
    if split_kernel is not None:
        operands += [split_kernel]
        out += [jax.ShapeDtypeStruct((copies, pairs, split_kernel.shape[1]), f32)]
        flops += 3 * pairs * split_kernel.size
    return pl.pallas_call(
        new_right if split_kernel is None else value_body,
        in_specs=[WHOLE] * len(operands),
        out_specs=[WHOLE] * len(out),
        out_shape=out,
        compiler_params=PARAMS,
        cost_estimate=cost(flops, *operands, *out),
        name="right" if split_kernel is None else "value",
    )(*operands)


def sum_body(pieces_ref, copies_ref):
    total = pieces_ref[0]
    for i in range(1, pieces_ref.shape[0]):
        total = total + pieces_ref[i]
    for i in range(copies_ref.shape[0]):
        copies_ref[i] = total


def summed(pieces, copies):
    out = jax.ShapeDtypeStruct((copies, *pieces.shape[1:]), f32)
    return pl.pallas_call(
        sum_body,
        in_specs=[WHOLE],
        out_specs=WHOLE,
        out_shape=out,
        compiler_params=PARAMS,
        cost_estimate=cost(pieces.size, pieces, out),
        name="sum",
    )(pieces)


def exchange(pieces, axis, groups=None):
    return lax.all_to_all(
        pieces, axis, split_axis=0, concat_axis=0, tiled=True, axis_index_groups=groups
    )


def from_everyone(array, axis, size):
    return exchange(jnp.broadcast_to(array, (size, *array.shape)), axis)


def solution(mesh):
    rows, cores = mesh.shape["row"], mesh.shape["rep"]
    far = rows // NEAR
    block = ("col", "rep")
    blocks = mesh.shape["col"] * cores
    lines = ("row", "rep")

    def device(row, core):
        return (row + core * NEAR // cores) % rows * cores + core

    near_groups = [
        [device(start + i, core) for i in range(NEAR)]
        for core in range(cores)
        for start in range(0, rows, NEAR)
    ]
    far_groups = [
        [device(start + i, core) for start in range(0, rows, NEAR)]
        for core in range(cores)
        for i in range(NEAR)
    ]

    def total_over_rows(pieces):
        pieces = summed(exchange(pieces, lines, near_groups), far)
        pieces = summed(exchange(pieces, lines, far_groups), NEAR)
        return exchange(pieces, lines, near_groups)

    def local(kernel, source, target):
        split_kernel, sums = split(kernel)
        values = from_everyone(sums, block, blocks)
        right_scale = jnp.ones(target.shape, f32)
        terms = []
        for step in range(ITERS):
            left_scale, pieces = scale_left(values, source, split_kernel)
            totals = total_over_rows(pieces)
            if step < ITERS - 1:
                right_scale, term, values = scale_right(
                    totals, target, right_scale, split_kernel, blocks
                )
                values = exchange(values, block)
            else:
                right_scale, term = scale_right(totals, target, right_scale)
            terms.append(term.reshape(-1))
        count = blocks * target.shape[1]
        errors = from_everyone(jnp.stack(terms), block, blocks).sum(axis=0) / count
        return left_scale, right_scale, errors

    return jax.shard_map(
        local,
        mesh=mesh,
        in_specs=(P(("groups", "row"), block), P("groups", "row"), P("groups", block)),
        out_specs=(P("groups", "row"), P("groups", block), P("groups", None)),
        check_vma=False,
    )
```

```python
import functools

import jax
import jax.numpy as jnp
from jax import lax
from jax.experimental import pallas as pl
from jax.experimental.pallas import tpu as pltpu
from jax.sharding import PartitionSpec as P

ITERS = 3
NEAR = 8
SPLIT_STEPS = 4
LANES = 128
SUBLANES = 8
f32 = jnp.float32
bf16 = jnp.bfloat16
WHOLE = pl.BlockSpec(memory_space=pltpu.VMEM)
PARAMS = pltpu.CompilerParams(vmem_limit_bytes=8 * 2**20)
BY_LAST = (((1,), (1,)), ((), ()))


def halves(array):
    high = array.astype(bf16)
    return high, (array - high.astype(f32)).astype(bf16)


def cost(flops, *arrays):
    moved = sum(a.size * a.dtype.itemsize for a in arrays)
    return pl.CostEstimate(flops=flops, bytes_accessed=moved, transcendentals=0)


def split_body(kernel_ref, halves_ref, sums_ref):
    kernel = kernel_ref[...]
    halves_ref[0], halves_ref[1] = halves(kernel)
    part = kernel[:, :LANES]
    for start in range(LANES, kernel.shape[1], LANES):
        part = part + kernel[:, start : start + LANES]
    sums = jnp.sum(part.T, axis=0, keepdims=True)
    for i in range(sums_ref.shape[0]):
        sums_ref[i] = sums


def split(kernel, copies):
    rows, columns = kernel.shape
    tile = rows // SPLIT_STEPS
    out = [
        jax.ShapeDtypeStruct((2, rows, columns), bf16),
        jax.ShapeDtypeStruct((copies, 1, rows), f32),
    ]
    return pl.pallas_call(
        split_body,
        grid=(SPLIT_STEPS,),
        in_specs=[pl.BlockSpec((tile, columns), lambda i: (i, 0))],
        out_specs=[
            pl.BlockSpec((2, tile, columns), lambda i: (0, i, 0)),
            pl.BlockSpec((copies, 1, tile), lambda i: (0, 0, i)),
        ],
        out_shape=out,
        compiler_params=PARAMS,
        cost_estimate=cost(4 * kernel.size, kernel, *out),
        name="split",
    )(kernel)


def back_body(value_ref, source_ref, halves_ref, left_ref, back_ref):
    value = value_ref[0]
    for i in range(1, value_ref.shape[0]):
        value = value + value_ref[i]
    left = source_ref[...] / value
    left_ref[...] = left
    high, low = halves(left)
    both = jnp.concatenate([high, low], axis=0)
    pairs = left.shape[0]
    width = back_ref.shape[2]
    for m in range(back_ref.shape[0]):
        here = slice(m * width, (m + 1) * width)
        first = jnp.dot(both, halves_ref[0, :, here], preferred_element_type=f32)
        second = jnp.dot(high, halves_ref[1, :, here], preferred_element_type=f32)
        back_ref[m] = first[:pairs] + first[pairs:] + second


def scale_left(values, source, split_kernel):
    pairs, rows = source.shape
    columns = split_kernel.shape[2]
    pieces = jax.ShapeDtypeStruct((NEAR, pairs, columns // NEAR), f32)
    return pl.pallas_call(
        back_body,
        in_specs=[WHOLE] * 3,
        out_specs=[WHOLE] * 2,
        out_shape=[jax.ShapeDtypeStruct((pairs, rows), f32), pieces],
        compiler_params=PARAMS,
        cost_estimate=cost(3 * pairs * split_kernel.size, values, source, split_kernel, pieces),
        name="back",
    )(values, source, split_kernel)


def new_right(total_ref, target_ref, old_ref, right_ref):
    pairs = target_ref.shape[0]
    width = total_ref.shape[2]
    error = jnp.zeros((pairs, width), f32)
    for m in range(total_ref.shape[0]):
        here = slice(m * width, (m + 1) * width)
        total = total_ref[m]
        target = target_ref[:, here]
        right_ref[:, here] = target / total
        error = error + jnp.abs(old_ref[:, here] * total - target)
    return jnp.sum(error, axis=1, keepdims=True)


def value_body(total_ref, target_ref, old_ref, halves_ref, right_ref, error_ref, value_ref):
    error_ref[...] = new_right(total_ref, target_ref, old_ref, right_ref)
    pairs = target_ref.shape[0]
    high, low = halves(right_ref[...])
    both = jnp.concatenate([high, low], axis=0)
    first = lax.dot_general(both, halves_ref[0], BY_LAST, preferred_element_type=f32)
    second = lax.dot_general(high, halves_ref[1], BY_LAST, preferred_element_type=f32)
    value = first[:pairs] + first[pairs:] + second
    for i in range(value_ref.shape[0]):
        value_ref[i] = value


def scale_right(totals, target, old, split_kernel, copies):
    pairs = target.shape[0]
    out = [
        jax.ShapeDtypeStruct(target.shape, f32),
        jax.ShapeDtypeStruct((pairs, 1), f32),
        jax.ShapeDtypeStruct((copies, pairs, split_kernel.shape[1]), f32),
    ]
    operands = [totals, target, old, split_kernel]
    return pl.pallas_call(
        value_body,
        in_specs=[WHOLE] * 4,
        out_specs=[WHOLE] * 3,
        out_shape=out,
        compiler_params=PARAMS,
        cost_estimate=cost(3 * pairs * split_kernel.size, *operands, *out),
        name="value",
    )(*operands)


def sum_body(pieces_ref, copies_ref):
    total = pieces_ref[0]
    for i in range(1, pieces_ref.shape[0]):
        total = total + pieces_ref[i]
    for i in range(copies_ref.shape[0]):
        copies_ref[i] = total


def summed(pieces, copies):
    out = jax.ShapeDtypeStruct((copies, *pieces.shape[1:]), f32)
    return pl.pallas_call(
        sum_body,
        in_specs=[WHOLE],
        out_specs=WHOLE,
        out_shape=out,
        compiler_params=PARAMS,
        cost_estimate=cost(pieces.size, pieces, out),
        name="sum",
    )(pieces)


def last_body(total_ref, target_ref, old_ref, *refs):
    *terms, right_ref, errors_ref = refs
    error = new_right(total_ref, target_ref, old_ref, right_ref)
    lane = lax.broadcasted_iota(jnp.int32, (error.shape[0], LANES), 1)
    table = jnp.zeros((error.shape[0], LANES), f32)
    for i, term in enumerate([*(t[...] for t in terms), error]):
        table = jnp.where(lane == i, term, table)
    rest = jnp.zeros((LANES - table.shape[0], LANES), f32)
    table = jnp.concatenate([table, rest], axis=0).T[: errors_ref.shape[1]]
    for i in range(errors_ref.shape[0]):
        errors_ref[i] = table


def last_right(totals, target, old, terms, copies):
    pairs = target.shape[0]
    out = [
        jax.ShapeDtypeStruct(target.shape, f32),
        jax.ShapeDtypeStruct((copies, SUBLANES, LANES), f32),
    ]
    operands = [totals, target, old, *terms]
    return pl.pallas_call(
        last_body,
        in_specs=[WHOLE] * len(operands),
        out_specs=[WHOLE] * 2,
        out_shape=out,
        compiler_params=PARAMS,
        cost_estimate=cost(4 * target.size, *operands, *out),
        name="last",
    )(*operands)


def errors_body(count, tables_ref, errors_ref):
    table = tables_ref[0]
    for i in range(1, tables_ref.shape[0]):
        table = table + tables_ref[i]
    errors_ref[...] = table[: errors_ref.shape[0], : errors_ref.shape[1]] / count


def mean_errors(tables, pairs, count):
    out = jax.ShapeDtypeStruct((ITERS, pairs), f32)
    return pl.pallas_call(
        functools.partial(errors_body, count),
        in_specs=[WHOLE],
        out_specs=WHOLE,
        out_shape=out,
        compiler_params=PARAMS,
        cost_estimate=cost(tables.size, tables, out),
        name="errors",
    )(tables)


def exchange(pieces, axis, groups=None):
    return lax.all_to_all(
        pieces, axis, split_axis=0, concat_axis=0, tiled=True, axis_index_groups=groups
    )


def solution(mesh):
    rows, cores = mesh.shape["row"], mesh.shape["rep"]
    far = rows // NEAR
    block = ("col", "rep")
    blocks = mesh.shape["col"] * cores
    lines = ("row", "rep")

    def device(row, core):
        return (row + core * NEAR // cores) % rows * cores + core

    def groups_of(members):
        return [[device(row, core) for row in rows_of] for core in range(cores) for rows_of in members]

    half = NEAR // 2
    starts = range(0, rows, NEAR)
    sum_groups = groups_of([[start + i for i in range(NEAR)] for start in starts])
    far_groups = groups_of([[start + i for start in starts] for i in range(NEAR)])
    gather_groups = groups_of(
        [[start + i + (NEAR if i < half else 0) for i in range(NEAR)] for start in starts]
    )

    def total_over_rows(pieces):
        pieces = summed(exchange(pieces, lines, sum_groups), far)
        pieces = summed(exchange(pieces, lines, far_groups), NEAR)
        return exchange(pieces, lines, gather_groups)

    def local(kernel, source, target):
        split_kernel, sums = split(kernel, blocks)
        values = exchange(sums, block)
        right_scale = jnp.ones(target.shape, f32)
        terms = []
        for step in range(ITERS):
            left_scale, pieces = scale_left(values, source, split_kernel)
            totals = total_over_rows(pieces)
            if step < ITERS - 1:
                right_scale, term, values = scale_right(
                    totals, target, right_scale, split_kernel, blocks
                )
                values = exchange(values, block)
                terms.append(term)
        right_scale, tables = last_right(totals, target, right_scale, terms, blocks)
        count = float(blocks * target.shape[1])
        errors = mean_errors(exchange(tables, block), target.shape[0], count)
        return left_scale, right_scale, errors

    return jax.shard_map(
        local,
        mesh=mesh,
        in_specs=(P(("groups", "row"), block), P("groups", "row"), P("groups", block)),
        out_specs=(P("groups", "row"), P("groups", block), P("groups", None)),
        check_vma=False,
    )
```

```python
import functools

import jax
import jax.numpy as jnp
from jax import lax
from jax.experimental import pallas as pl
from jax.experimental.pallas import tpu as pltpu
from jax.sharding import PartitionSpec as P

ITERS = 3
NEAR = 8
SPLIT_STEPS = 4
LANES = 128
SUBLANES = 8
f32 = jnp.float32
bf16 = jnp.bfloat16
WHOLE = pl.BlockSpec(memory_space=pltpu.VMEM)
PARAMS = pltpu.CompilerParams(vmem_limit_bytes=8 * 2**20)
BY_LAST = (((1,), (1,)), ((), ()))


def halves(array):
    high = array.astype(bf16)
    return high, (array - high.astype(f32)).astype(bf16)


def cost(flops, *arrays):
    moved = sum(a.size * a.dtype.itemsize for a in arrays)
    return pl.CostEstimate(flops=flops, bytes_accessed=moved, transcendentals=0)


def split_body(kernel_ref, halves_ref, sums_ref):
    kernel = kernel_ref[...]
    halves_ref[0], halves_ref[1] = halves(kernel)
    part = kernel[:, :LANES]
    for start in range(LANES, kernel.shape[1], LANES):
        part = part + kernel[:, start : start + LANES]
    sums = jnp.sum(part.T, axis=0, keepdims=True)
    for i in range(sums_ref.shape[0]):
        sums_ref[i] = sums


def split(kernel, copies):
    rows, columns = kernel.shape
    tile = rows // SPLIT_STEPS
    out = [
        jax.ShapeDtypeStruct((2, rows, columns), bf16),
        jax.ShapeDtypeStruct((copies, 1, rows), f32),
    ]
    return pl.pallas_call(
        split_body,
        grid=(SPLIT_STEPS,),
        in_specs=[pl.BlockSpec((tile, columns), lambda i: (i, 0))],
        out_specs=[
            pl.BlockSpec((2, tile, columns), lambda i: (0, i, 0)),
            pl.BlockSpec((copies, 1, tile), lambda i: (0, 0, i)),
        ],
        out_shape=out,
        compiler_params=PARAMS,
        cost_estimate=cost(4 * kernel.size, kernel, *out),
        name="split",
    )(kernel)


def back_body(value_ref, source_ref, halves_ref, left_ref, back_ref):
    value = value_ref[0]
    for i in range(1, value_ref.shape[0]):
        value = value + value_ref[i]
    left = source_ref[...] / value
    left_ref[...] = left
    high, low = halves(left)
    both = jnp.concatenate([high, low], axis=0)
    pairs = left.shape[0]
    width = back_ref.shape[2]
    for m in range(back_ref.shape[0]):
        here = slice(m * width, (m + 1) * width)
        first = jnp.dot(both, halves_ref[0, :, here], preferred_element_type=f32)
        second = jnp.dot(high, halves_ref[1, :, here], preferred_element_type=f32)
        back_ref[m] = first[:pairs] + first[pairs:] + second


def scale_left(values, source, split_kernel):
    pairs, rows = source.shape
    columns = split_kernel.shape[2]
    pieces = jax.ShapeDtypeStruct((NEAR, pairs, columns // NEAR), f32)
    return pl.pallas_call(
        back_body,
        in_specs=[WHOLE] * 3,
        out_specs=[WHOLE] * 2,
        out_shape=[jax.ShapeDtypeStruct((pairs, rows), f32), pieces],
        compiler_params=PARAMS,
        cost_estimate=cost(3 * pairs * split_kernel.size, values, source, split_kernel, pieces),
        name="back",
    )(values, source, split_kernel)


def new_right(total_ref, target_ref, old_ref, right_ref):
    pairs = target_ref.shape[0]
    width = total_ref.shape[2]
    error = jnp.zeros((pairs, width), f32)
    for m in range(total_ref.shape[0]):
        here = slice(m * width, (m + 1) * width)
        total = total_ref[m]
        target = target_ref[:, here]
        right_ref[:, here] = target / total
        error = error + jnp.abs(old_ref[:, here] * total - target)
    return jnp.sum(error, axis=1, keepdims=True)


def value_body(total_ref, target_ref, old_ref, halves_ref, right_ref, error_ref, value_ref):
    error_ref[...] = new_right(total_ref, target_ref, old_ref, right_ref)
    pairs = target_ref.shape[0]
    high, low = halves(right_ref[...])
    both = jnp.concatenate([high, low], axis=0)
    first = lax.dot_general(both, halves_ref[0], BY_LAST, preferred_element_type=f32)
    second = lax.dot_general(high, halves_ref[1], BY_LAST, preferred_element_type=f32)
    value = first[:pairs] + first[pairs:] + second
    for i in range(value_ref.shape[0]):
        value_ref[i] = value


def scale_right(totals, target, old, split_kernel, copies):
    pairs = target.shape[0]
    out = [
        jax.ShapeDtypeStruct(target.shape, f32),
        jax.ShapeDtypeStruct((pairs, 1), f32),
        jax.ShapeDtypeStruct((copies, pairs, split_kernel.shape[1]), f32),
    ]
    operands = [totals, target, old, split_kernel]
    return pl.pallas_call(
        value_body,
        in_specs=[WHOLE] * 4,
        out_specs=[WHOLE] * 3,
        out_shape=out,
        compiler_params=PARAMS,
        cost_estimate=cost(3 * pairs * split_kernel.size, *operands, *out),
        name="value",
    )(*operands)


def sum_body(pieces_ref, copies_ref):
    total = pieces_ref[0]
    for i in range(1, pieces_ref.shape[0]):
        total = total + pieces_ref[i]
    for i in range(copies_ref.shape[0]):
        copies_ref[i] = total


def summed(pieces, copies):
    out = jax.ShapeDtypeStruct((copies, *pieces.shape[1:]), f32)
    return pl.pallas_call(
        sum_body,
        in_specs=[WHOLE],
        out_specs=WHOLE,
        out_shape=out,
        compiler_params=PARAMS,
        cost_estimate=cost(pieces.size, pieces, out),
        name="sum",
    )(pieces)


def last_body(total_ref, target_ref, old_ref, *refs):
    *terms, right_ref, errors_ref = refs
    error = new_right(total_ref, target_ref, old_ref, right_ref)
    lane = lax.broadcasted_iota(jnp.int32, (error.shape[0], LANES), 1)
    table = jnp.zeros((error.shape[0], LANES), f32)
    for i, term in enumerate([*(t[...] for t in terms), error]):
        table = jnp.where(lane == i, term, table)
    rest = jnp.zeros((LANES - table.shape[0], LANES), f32)
    table = jnp.concatenate([table, rest], axis=0).T[: errors_ref.shape[1]]
    for i in range(errors_ref.shape[0]):
        errors_ref[i] = table


def last_right(totals, target, old, terms, copies):
    pairs = target.shape[0]
    out = [
        jax.ShapeDtypeStruct(target.shape, f32),
        jax.ShapeDtypeStruct((copies, SUBLANES, LANES), f32),
    ]
    operands = [totals, target, old, *terms]
    return pl.pallas_call(
        last_body,
        in_specs=[WHOLE] * len(operands),
        out_specs=[WHOLE] * 2,
        out_shape=out,
        compiler_params=PARAMS,
        cost_estimate=cost(4 * target.size, *operands, *out),
        name="last",
    )(*operands)


def errors_body(count, tables_ref, errors_ref):
    table = tables_ref[0]
    for i in range(1, tables_ref.shape[0]):
        table = table + tables_ref[i]
    errors_ref[...] = table[: errors_ref.shape[0], : errors_ref.shape[1]] / count


def mean_errors(tables, pairs, count):
    out = jax.ShapeDtypeStruct((ITERS, pairs), f32)
    return pl.pallas_call(
        functools.partial(errors_body, count),
        in_specs=[WHOLE],
        out_specs=WHOLE,
        out_shape=out,
        compiler_params=PARAMS,
        cost_estimate=cost(tables.size, tables, out),
        name="errors",
    )(tables)


def exchange(pieces, axis, groups=None):
    return lax.all_to_all(
        pieces, axis, split_axis=0, concat_axis=0, tiled=True, axis_index_groups=groups
    )


def solution(mesh):
    rows, cores = mesh.shape["row"], mesh.shape["rep"]
    far = rows // NEAR
    block = ("col", "rep")
    blocks = mesh.shape["col"] * cores
    lines = ("row", "rep")

    def device(row, core):
        return (row + core * NEAR // cores) % rows * cores + core

    def groups_of(members):
        return [[device(row, core) for row in rows_of] for core in range(cores) for rows_of in members]

    half = NEAR // 2

    def owner(group, piece):
        moved = half // 2 if group % far >= far // 2 else 0
        return group * NEAR + piece // half * half + (piece + moved) % half

    pieces_of, groups = range(NEAR), range(far)
    sum_groups = groups_of([[owner(g, m) for m in pieces_of] for g in groups])
    far_groups = groups_of([[owner(g, m) for g in groups] for m in pieces_of])
    gather_groups = groups_of([[owner(g + (m < half), m) for m in pieces_of] for g in groups])

    def total_over_rows(pieces):
        pieces = summed(exchange(pieces, lines, sum_groups), far)
        pieces = summed(exchange(pieces, lines, far_groups), NEAR)
        return exchange(pieces, lines, gather_groups)

    def local(kernel, source, target):
        split_kernel, sums = split(kernel, blocks)
        values = exchange(sums, block)
        right_scale = jnp.ones(target.shape, f32)
        terms = []
        for step in range(ITERS):
            left_scale, pieces = scale_left(values, source, split_kernel)
            totals = total_over_rows(pieces)
            if step < ITERS - 1:
                right_scale, term, values = scale_right(
                    totals, target, right_scale, split_kernel, blocks
                )
                values = exchange(values, block)
                terms.append(term)
        right_scale, tables = last_right(totals, target, right_scale, terms, blocks)
        count = float(blocks * target.shape[1])
        errors = mean_errors(exchange(tables, block), target.shape[0], count)
        return left_scale, right_scale, errors

    return jax.shard_map(
        local,
        mesh=mesh,
        in_specs=(P(("groups", "row"), block), P("groups", "row"), P("groups", block)),
        out_specs=(P("groups", "row"), P("groups", block), P("groups", None)),
        check_vma=False,
    )
```

```python
import functools

import jax
import jax.numpy as jnp
from jax import lax
from jax.experimental import pallas as pl
from jax.experimental.pallas import tpu as pltpu
from jax.sharding import PartitionSpec as P

ITERS = 3
NEAR = 8
OWNERS = (
    (2, 5, 4, 7, 1, 6, 0, 3),
    (3, 1, 5, 6, 0, 7, 2, 4),
    (4, 0, 2, 1, 6, 3, 5, 7),
    (5, 4, 1, 7, 2, 0, 3, 6),
)
SPLIT_STEPS = 4
LANES = 128
SUBLANES = 8
f32 = jnp.float32
bf16 = jnp.bfloat16
WHOLE = pl.BlockSpec(memory_space=pltpu.VMEM)
PARAMS = pltpu.CompilerParams(vmem_limit_bytes=8 * 2**20)
BY_LAST = (((1,), (1,)), ((), ()))


def halves(array):
    high = array.astype(bf16)
    return high, (array - high.astype(f32)).astype(bf16)


def cost(flops, *arrays):
    moved = sum(a.size * a.dtype.itemsize for a in arrays)
    return pl.CostEstimate(flops=flops, bytes_accessed=moved, transcendentals=0)


def split_body(kernel_ref, halves_ref, sums_ref):
    kernel = kernel_ref[...]
    halves_ref[0], halves_ref[1] = halves(kernel)
    part = kernel[:, :LANES]
    for start in range(LANES, kernel.shape[1], LANES):
        part = part + kernel[:, start : start + LANES]
    sums = jnp.sum(part.T, axis=0, keepdims=True)
    for i in range(sums_ref.shape[0]):
        sums_ref[i] = sums


def split(kernel, copies):
    rows, columns = kernel.shape
    tile = rows // SPLIT_STEPS
    out = [
        jax.ShapeDtypeStruct((2, rows, columns), bf16),
        jax.ShapeDtypeStruct((copies, 1, rows), f32),
    ]
    return pl.pallas_call(
        split_body,
        grid=(SPLIT_STEPS,),
        in_specs=[pl.BlockSpec((tile, columns), lambda i: (i, 0))],
        out_specs=[
            pl.BlockSpec((2, tile, columns), lambda i: (0, i, 0)),
            pl.BlockSpec((copies, 1, tile), lambda i: (0, 0, i)),
        ],
        out_shape=out,
        compiler_params=PARAMS,
        cost_estimate=cost(4 * kernel.size, kernel, *out),
        name="split",
    )(kernel)


def back_body(value_ref, source_ref, halves_ref, left_ref, back_ref):
    value = value_ref[0]
    for i in range(1, value_ref.shape[0]):
        value = value + value_ref[i]
    left = source_ref[...] / value
    left_ref[...] = left
    high, low = halves(left)
    both = jnp.concatenate([high, low], axis=0)
    pairs = left.shape[0]
    width = back_ref.shape[2]
    for m in range(back_ref.shape[0]):
        here = slice(m * width, (m + 1) * width)
        first = jnp.dot(both, halves_ref[0, :, here], preferred_element_type=f32)
        second = jnp.dot(high, halves_ref[1, :, here], preferred_element_type=f32)
        back_ref[m] = first[:pairs] + first[pairs:] + second


def scale_left(values, source, split_kernel):
    pairs, rows = source.shape
    columns = split_kernel.shape[2]
    pieces = jax.ShapeDtypeStruct((NEAR, pairs, columns // NEAR), f32)
    return pl.pallas_call(
        back_body,
        in_specs=[WHOLE] * 3,
        out_specs=[WHOLE] * 2,
        out_shape=[jax.ShapeDtypeStruct((pairs, rows), f32), pieces],
        compiler_params=PARAMS,
        cost_estimate=cost(3 * pairs * split_kernel.size, values, source, split_kernel, pieces),
        name="back",
    )(values, source, split_kernel)


def new_right(total_ref, target_ref, old_ref, right_ref):
    pairs = target_ref.shape[0]
    width = total_ref.shape[2]
    error = jnp.zeros((pairs, width), f32)
    for m in range(total_ref.shape[0]):
        here = slice(m * width, (m + 1) * width)
        total = total_ref[m]
        target = target_ref[:, here]
        right_ref[:, here] = target / total
        error = error + jnp.abs(old_ref[:, here] * total - target)
    return jnp.sum(error, axis=1, keepdims=True)


def value_body(total_ref, target_ref, old_ref, halves_ref, right_ref, error_ref, value_ref):
    error_ref[...] = new_right(total_ref, target_ref, old_ref, right_ref)
    pairs = target_ref.shape[0]
    high, low = halves(right_ref[...])
    both = jnp.concatenate([high, low], axis=0)
    first = lax.dot_general(both, halves_ref[0], BY_LAST, preferred_element_type=f32)
    second = lax.dot_general(high, halves_ref[1], BY_LAST, preferred_element_type=f32)
    value = first[:pairs] + first[pairs:] + second
    for i in range(value_ref.shape[0]):
        value_ref[i] = value


def scale_right(totals, target, old, split_kernel, copies):
    pairs = target.shape[0]
    out = [
        jax.ShapeDtypeStruct(target.shape, f32),
        jax.ShapeDtypeStruct((pairs, 1), f32),
        jax.ShapeDtypeStruct((copies, pairs, split_kernel.shape[1]), f32),
    ]
    operands = [totals, target, old, split_kernel]
    return pl.pallas_call(
        value_body,
        in_specs=[WHOLE] * 4,
        out_specs=[WHOLE] * 3,
        out_shape=out,
        compiler_params=PARAMS,
        cost_estimate=cost(3 * pairs * split_kernel.size, *operands, *out),
        name="value",
    )(*operands)


def sum_body(pieces_ref, copies_ref):
    total = pieces_ref[0]
    for i in range(1, pieces_ref.shape[0]):
        total = total + pieces_ref[i]
    for i in range(copies_ref.shape[0]):
        copies_ref[i] = total


def summed(pieces, copies):
    out = jax.ShapeDtypeStruct((copies, *pieces.shape[1:]), f32)
    return pl.pallas_call(
        sum_body,
        in_specs=[WHOLE],
        out_specs=WHOLE,
        out_shape=out,
        compiler_params=PARAMS,
        cost_estimate=cost(pieces.size, pieces, out),
        name="sum",
    )(pieces)


def last_body(total_ref, target_ref, old_ref, *refs):
    *terms, right_ref, errors_ref = refs
    error = new_right(total_ref, target_ref, old_ref, right_ref)
    lane = lax.broadcasted_iota(jnp.int32, (error.shape[0], LANES), 1)
    table = jnp.zeros((error.shape[0], LANES), f32)
    for i, term in enumerate([*(t[...] for t in terms), error]):
        table = jnp.where(lane == i, term, table)
    rest = jnp.zeros((LANES - table.shape[0], LANES), f32)
    table = jnp.concatenate([table, rest], axis=0).T[: errors_ref.shape[1]]
    for i in range(errors_ref.shape[0]):
        errors_ref[i] = table


def last_right(totals, target, old, terms, copies):
    pairs = target.shape[0]
    out = [
        jax.ShapeDtypeStruct(target.shape, f32),
        jax.ShapeDtypeStruct((copies, SUBLANES, LANES), f32),
    ]
    operands = [totals, target, old, *terms]
    return pl.pallas_call(
        last_body,
        in_specs=[WHOLE] * len(operands),
        out_specs=[WHOLE] * 2,
        out_shape=out,
        compiler_params=PARAMS,
        cost_estimate=cost(4 * target.size, *operands, *out),
        name="last",
    )(*operands)


def errors_body(count, tables_ref, errors_ref):
    table = tables_ref[0]
    for i in range(1, tables_ref.shape[0]):
        table = table + tables_ref[i]
    errors_ref[...] = table[: errors_ref.shape[0], : errors_ref.shape[1]] / count


def mean_errors(tables, pairs, count):
    out = jax.ShapeDtypeStruct((ITERS, pairs), f32)
    return pl.pallas_call(
        functools.partial(errors_body, count),
        in_specs=[WHOLE],
        out_specs=WHOLE,
        out_shape=out,
        compiler_params=PARAMS,
        cost_estimate=cost(tables.size, tables, out),
        name="errors",
    )(tables)


def exchange(pieces, axis, groups=None):
    return lax.all_to_all(
        pieces, axis, split_axis=0, concat_axis=0, tiled=True, axis_index_groups=groups
    )


def solution(mesh):
    rows, cores = mesh.shape["row"], mesh.shape["rep"]
    far = rows // NEAR
    block = ("col", "rep")
    blocks = mesh.shape["col"] * cores
    lines = ("row", "rep")

    def device(row, core):
        return (row + core * NEAR // cores) % rows * cores + core

    def groups_of(members):
        return [[device(row, core) for row in rows_of] for core in range(cores) for rows_of in members]

    def apart(one, other):
        return min((one - other) % rows, (other - one) % rows)

    def longest(first, members):
        entry = max(apart(k, first) for k in members)
        return entry + max(apart(first, k) + apart(k, j) for k in members for j in members)

    def first_chosen(members):
        first = min(members, key=lambda row: longest(row, members))
        return [first] + [row for row in members if row != first]

    def owner(group, piece):
        return group * NEAR + OWNERS[group][piece]

    near_groups = groups_of([[owner(g, m) for m in range(NEAR)] for g in range(far)])
    far_groups = groups_of(
        [first_chosen([owner(g, m) for g in range(far)]) for m in range(NEAR)]
    )

    def total_over_rows(pieces):
        pieces = summed(exchange(pieces, lines, near_groups), far)
        pieces = summed(exchange(pieces, lines, far_groups), NEAR)
        return exchange(pieces, lines, near_groups)

    def local(kernel, source, target):
        split_kernel, sums = split(kernel, blocks)
        values = exchange(sums, block)
        right_scale = jnp.ones(target.shape, f32)
        terms = []
        for step in range(ITERS):
            left_scale, pieces = scale_left(values, source, split_kernel)
            totals = total_over_rows(pieces)
            if step < ITERS - 1:
                right_scale, term, values = scale_right(
                    totals, target, right_scale, split_kernel, blocks
                )
                values = exchange(values, block)
                terms.append(term)
        right_scale, tables = last_right(totals, target, right_scale, terms, blocks)
        count = float(blocks * target.shape[1])
        errors = mean_errors(exchange(tables, block), target.shape[0], count)
        return left_scale, right_scale, errors

    return jax.shard_map(
        local,
        mesh=mesh,
        in_specs=(P(("groups", "row"), block), P("groups", "row"), P("groups", block)),
        out_specs=(P("groups", "row"), P("groups", block), P("groups", None)),
        check_vma=False,
    )
```

```python
import functools

import jax
import jax.numpy as jnp
from jax import lax
from jax.experimental import pallas as pl
from jax.experimental.pallas import tpu as pltpu
from jax.sharding import PartitionSpec as P

ITERS = 3
NEAR = 8
OWNERS = (
    (3, 7, 1, 4, 0, 5, 6, 2),
    (3, 0, 2, 7, 1, 6, 5, 4),
    (5, 3, 6, 2, 4, 0, 1, 7),
    (5, 4, 7, 3, 6, 2, 1, 0),
)
FAR_FIRST = (
    (3, 3, 3, 3, 3, 3, 3, 3),
    (3, 3, 3, 3, 3, 2, 2, 2),
)
SPLIT_STEPS = 4
LANES = 128
SUBLANES = 8
f32 = jnp.float32
bf16 = jnp.bfloat16
WHOLE = pl.BlockSpec(memory_space=pltpu.VMEM)
PARAMS = pltpu.CompilerParams(vmem_limit_bytes=8 * 2**20)
BY_LAST = (((1,), (1,)), ((), ()))


def halves(array):
    high = array.astype(bf16)
    return high, (array - high.astype(f32)).astype(bf16)


def cost(flops, *arrays):
    moved = sum(a.size * a.dtype.itemsize for a in arrays)
    return pl.CostEstimate(flops=flops, bytes_accessed=moved, transcendentals=0)


def split_body(kernel_ref, halves_ref, sums_ref):
    kernel = kernel_ref[...]
    halves_ref[0], halves_ref[1] = halves(kernel)
    part = kernel[:, :LANES]
    for start in range(LANES, kernel.shape[1], LANES):
        part = part + kernel[:, start : start + LANES]
    sums = jnp.sum(part.T, axis=0, keepdims=True)
    for i in range(sums_ref.shape[0]):
        sums_ref[i] = sums


def split(kernel, copies):
    rows, columns = kernel.shape
    tile = rows // SPLIT_STEPS
    out = [
        jax.ShapeDtypeStruct((2, rows, columns), bf16),
        jax.ShapeDtypeStruct((copies, 1, rows), f32),
    ]
    return pl.pallas_call(
        split_body,
        grid=(SPLIT_STEPS,),
        in_specs=[pl.BlockSpec((tile, columns), lambda i: (i, 0))],
        out_specs=[
            pl.BlockSpec((2, tile, columns), lambda i: (0, i, 0)),
            pl.BlockSpec((copies, 1, tile), lambda i: (0, 0, i)),
        ],
        out_shape=out,
        compiler_params=PARAMS,
        cost_estimate=cost(4 * kernel.size, kernel, *out),
        name="split",
    )(kernel)


def back_body(value_ref, source_ref, halves_ref, left_ref, back_ref):
    value = value_ref[0]
    for i in range(1, value_ref.shape[0]):
        value = value + value_ref[i]
    left = source_ref[...] / value
    left_ref[...] = left
    high, low = halves(left)
    both = jnp.concatenate([high, low], axis=0)
    pairs = left.shape[0]
    width = back_ref.shape[2]
    for m in range(back_ref.shape[0]):
        here = slice(m * width, (m + 1) * width)
        first = jnp.dot(both, halves_ref[0, :, here], preferred_element_type=f32)
        second = jnp.dot(high, halves_ref[1, :, here], preferred_element_type=f32)
        back_ref[m] = first[:pairs] + first[pairs:] + second


def scale_left(values, source, split_kernel):
    pairs, rows = source.shape
    columns = split_kernel.shape[2]
    pieces = jax.ShapeDtypeStruct((NEAR, pairs, columns // NEAR), f32)
    return pl.pallas_call(
        back_body,
        in_specs=[WHOLE] * 3,
        out_specs=[WHOLE] * 2,
        out_shape=[jax.ShapeDtypeStruct((pairs, rows), f32), pieces],
        compiler_params=PARAMS,
        cost_estimate=cost(3 * pairs * split_kernel.size, values, source, split_kernel, pieces),
        name="back",
    )(values, source, split_kernel)


def new_right(total_ref, target_ref, old_ref, right_ref):
    pairs = target_ref.shape[0]
    width = total_ref.shape[2]
    error = jnp.zeros((pairs, width), f32)
    for m in range(total_ref.shape[0]):
        here = slice(m * width, (m + 1) * width)
        total = total_ref[m]
        target = target_ref[:, here]
        right_ref[:, here] = target / total
        error = error + jnp.abs(old_ref[:, here] * total - target)
    return jnp.sum(error, axis=1, keepdims=True)


def value_body(total_ref, target_ref, old_ref, halves_ref, right_ref, error_ref, value_ref):
    error_ref[...] = new_right(total_ref, target_ref, old_ref, right_ref)
    pairs = target_ref.shape[0]
    high, low = halves(right_ref[...])
    both = jnp.concatenate([high, low], axis=0)
    first = lax.dot_general(both, halves_ref[0], BY_LAST, preferred_element_type=f32)
    second = lax.dot_general(high, halves_ref[1], BY_LAST, preferred_element_type=f32)
    value = first[:pairs] + first[pairs:] + second
    for i in range(value_ref.shape[0]):
        value_ref[i] = value


def scale_right(totals, target, old, split_kernel, copies):
    pairs = target.shape[0]
    out = [
        jax.ShapeDtypeStruct(target.shape, f32),
        jax.ShapeDtypeStruct((pairs, 1), f32),
        jax.ShapeDtypeStruct((copies, pairs, split_kernel.shape[1]), f32),
    ]
    operands = [totals, target, old, split_kernel]
    return pl.pallas_call(
        value_body,
        in_specs=[WHOLE] * 4,
        out_specs=[WHOLE] * 3,
        out_shape=out,
        compiler_params=PARAMS,
        cost_estimate=cost(3 * pairs * split_kernel.size, *operands, *out),
        name="value",
    )(*operands)


def sum_body(pieces_ref, copies_ref):
    total = pieces_ref[0]
    for i in range(1, pieces_ref.shape[0]):
        total = total + pieces_ref[i]
    for i in range(copies_ref.shape[0]):
        copies_ref[i] = total


def summed(pieces, copies):
    out = jax.ShapeDtypeStruct((copies, *pieces.shape[1:]), f32)
    return pl.pallas_call(
        sum_body,
        in_specs=[WHOLE],
        out_specs=WHOLE,
        out_shape=out,
        compiler_params=PARAMS,
        cost_estimate=cost(pieces.size, pieces, out),
        name="sum",
    )(pieces)


def last_body(total_ref, target_ref, old_ref, *refs):
    *terms, right_ref, errors_ref = refs
    error = new_right(total_ref, target_ref, old_ref, right_ref)
    lane = lax.broadcasted_iota(jnp.int32, (error.shape[0], LANES), 1)
    table = jnp.zeros((error.shape[0], LANES), f32)
    for i, term in enumerate([*(t[...] for t in terms), error]):
        table = jnp.where(lane == i, term, table)
    rest = jnp.zeros((LANES - table.shape[0], LANES), f32)
    table = jnp.concatenate([table, rest], axis=0).T[: errors_ref.shape[1]]
    for i in range(errors_ref.shape[0]):
        errors_ref[i] = table


def last_right(totals, target, old, terms, copies):
    pairs = target.shape[0]
    out = [
        jax.ShapeDtypeStruct(target.shape, f32),
        jax.ShapeDtypeStruct((copies, SUBLANES, LANES), f32),
    ]
    operands = [totals, target, old, *terms]
    return pl.pallas_call(
        last_body,
        in_specs=[WHOLE] * len(operands),
        out_specs=[WHOLE] * 2,
        out_shape=out,
        compiler_params=PARAMS,
        cost_estimate=cost(4 * target.size, *operands, *out),
        name="last",
    )(*operands)


def errors_body(count, tables_ref, errors_ref):
    table = tables_ref[0]
    for i in range(1, tables_ref.shape[0]):
        table = table + tables_ref[i]
    errors_ref[...] = table[: errors_ref.shape[0], : errors_ref.shape[1]] / count


def mean_errors(tables, pairs, count):
    out = jax.ShapeDtypeStruct((ITERS, pairs), f32)
    return pl.pallas_call(
        functools.partial(errors_body, count),
        in_specs=[WHOLE],
        out_specs=WHOLE,
        out_shape=out,
        compiler_params=PARAMS,
        cost_estimate=cost(tables.size, tables, out),
        name="errors",
    )(tables)


def exchange(pieces, axis, groups=None):
    return lax.all_to_all(
        pieces, axis, split_axis=0, concat_axis=0, tiled=True, axis_index_groups=groups
    )


def solution(mesh):
    rows, cores = mesh.shape["row"], mesh.shape["rep"]
    far = rows // NEAR
    block = ("col", "rep")
    blocks = mesh.shape["col"] * cores
    lines = ("row", "rep")

    def device(row, core):
        return (row + core * NEAR // cores) % rows * cores + core

    def groups_of(members):
        return [[device(row, core) for row in rows_of] for core in range(cores) for rows_of in members]

    def owner(group, piece):
        return group * NEAR + OWNERS[group][piece]

    near_groups = groups_of([[owner(g, m) for m in range(NEAR)] for g in range(far)])
    far_groups = [
        groups_of(
            [[owner((first + i) % far, m) for i in range(far)] for m, first in enumerate(firsts)]
        )
        for firsts in FAR_FIRST
    ]

    def total_over_rows(pieces, step):
        pieces = summed(exchange(pieces, lines, near_groups), far)
        pieces = summed(exchange(pieces, lines, far_groups[min(step, 1)]), NEAR)
        return exchange(pieces, lines, near_groups)

    def local(kernel, source, target):
        split_kernel, sums = split(kernel, blocks)
        values = exchange(sums, block)
        right_scale = jnp.ones(target.shape, f32)
        terms = []
        for step in range(ITERS):
            left_scale, pieces = scale_left(values, source, split_kernel)
            totals = total_over_rows(pieces, step)
            if step < ITERS - 1:
                right_scale, term, values = scale_right(
                    totals, target, right_scale, split_kernel, blocks
                )
                values = exchange(values, block)
                terms.append(term)
        right_scale, tables = last_right(totals, target, right_scale, terms, blocks)
        count = float(blocks * target.shape[1])
        errors = mean_errors(exchange(tables, block), target.shape[0], count)
        return left_scale, right_scale, errors

    return jax.shard_map(
        local,
        mesh=mesh,
        in_specs=(P(("groups", "row"), block), P("groups", "row"), P("groups", block)),
        out_specs=(P("groups", "row"), P("groups", block), P("groups", None)),
        check_vma=False,
    )
```

```python
import functools

import jax
import jax.numpy as jnp
from jax import lax
from jax.experimental import pallas as pl
from jax.experimental.pallas import tpu as pltpu
from jax.sharding import PartitionSpec as P

ITERS = 3
NEAR = 8
OWNERS = (
    (3, 7, 1, 4, 0, 5, 6, 2),
    (3, 0, 2, 7, 1, 6, 5, 4),
    (5, 3, 6, 2, 4, 0, 1, 7),
    (5, 4, 7, 3, 6, 2, 1, 0),
)
FAR_FIRST = (
    (3, 3, 3, 3, 3, 3, 3, 3),
    (3, 3, 3, 3, 3, 2, 2, 2),
)
SPLIT_STEPS = 4
LANES = 128
SUBLANES = 8
f32 = jnp.float32
bf16 = jnp.bfloat16
WHOLE = pl.BlockSpec(memory_space=pltpu.VMEM)
PARAMS = pltpu.CompilerParams(vmem_limit_bytes=8 * 2**20)
BY_LAST = (((1,), (1,)), ((), ()))


def halves(array):
    high = array.astype(bf16)
    return high, (array - high.astype(f32)).astype(bf16)


def cost(flops, *arrays):
    moved = sum(a.size * a.dtype.itemsize for a in arrays)
    return pl.CostEstimate(flops=flops, bytes_accessed=moved, transcendentals=0)


def split_body(kernel_ref, halves_ref, sums_ref):
    kernel = kernel_ref[...]
    halves_ref[0], halves_ref[1] = halves(kernel)
    part = kernel[:, :LANES]
    for start in range(LANES, kernel.shape[1], LANES):
        part = part + kernel[:, start : start + LANES]
    sums = jnp.sum(part.T, axis=0, keepdims=True)
    for i in range(sums_ref.shape[0]):
        sums_ref[i] = sums


def split(kernel, copies):
    rows, columns = kernel.shape
    tile = rows // SPLIT_STEPS
    out = [
        jax.ShapeDtypeStruct((2, rows, columns), bf16),
        jax.ShapeDtypeStruct((copies, 1, rows), f32),
    ]
    return pl.pallas_call(
        split_body,
        grid=(SPLIT_STEPS,),
        in_specs=[pl.BlockSpec((tile, columns), lambda i: (i, 0))],
        out_specs=[
            pl.BlockSpec((2, tile, columns), lambda i: (0, i, 0)),
            pl.BlockSpec((copies, 1, tile), lambda i: (0, 0, i)),
        ],
        out_shape=out,
        compiler_params=PARAMS,
        cost_estimate=cost(4 * kernel.size, kernel, *out),
        name="split",
    )(kernel)


def back_body(value_ref, source_ref, halves_ref, left_ref, back_ref):
    value = value_ref[0]
    for i in range(1, value_ref.shape[0]):
        value = value + value_ref[i]
    left = source_ref[...] / value
    left_ref[...] = left
    high, low = halves(left)
    both = jnp.concatenate([high, low], axis=0)
    pairs = left.shape[0]
    width = back_ref.shape[2]
    for m in range(back_ref.shape[0]):
        here = slice(m * width, (m + 1) * width)
        first = jnp.dot(both, halves_ref[0, :, here], preferred_element_type=f32)
        second = jnp.dot(high, halves_ref[1, :, here], preferred_element_type=f32)
        back_ref[m] = first[:pairs] + first[pairs:] + second


def scale_left(values, source, split_kernel):
    pairs, rows = source.shape
    columns = split_kernel.shape[2]
    pieces = jax.ShapeDtypeStruct((NEAR, pairs, columns // NEAR), f32)
    return pl.pallas_call(
        back_body,
        in_specs=[WHOLE] * 3,
        out_specs=[WHOLE] * 2,
        out_shape=[jax.ShapeDtypeStruct((pairs, rows), f32), pieces],
        compiler_params=PARAMS,
        cost_estimate=cost(3 * pairs * split_kernel.size, values, source, split_kernel, pieces),
        name="back",
    )(values, source, split_kernel)


def new_right(total_ref, target_ref, old_ref, right_ref):
    pairs = target_ref.shape[0]
    width = total_ref.shape[2]
    error = jnp.zeros((pairs, width), f32)
    for m in range(total_ref.shape[0]):
        here = slice(m * width, (m + 1) * width)
        total = total_ref[m]
        target = target_ref[:, here]
        right_ref[:, here] = target / total
        error = error + jnp.abs(old_ref[:, here] * total - target)
    return jnp.sum(error, axis=1, keepdims=True)


def value_body(total_ref, target_ref, old_ref, halves_ref, right_ref, error_ref, value_ref):
    error_ref[...] = new_right(total_ref, target_ref, old_ref, right_ref)
    pairs = target_ref.shape[0]
    high, low = halves(right_ref[...])
    both = jnp.concatenate([high, low], axis=0)
    first = lax.dot_general(both, halves_ref[0], BY_LAST, preferred_element_type=f32)
    second = lax.dot_general(high, halves_ref[1], BY_LAST, preferred_element_type=f32)
    value = first[:pairs] + first[pairs:] + second
    for i in range(value_ref.shape[0]):
        value_ref[i] = value


def scale_right(totals, target, old, split_kernel, copies):
    pairs = target.shape[0]
    out = [
        jax.ShapeDtypeStruct(target.shape, f32),
        jax.ShapeDtypeStruct((pairs, 1), f32),
        jax.ShapeDtypeStruct((copies, pairs, split_kernel.shape[1]), f32),
    ]
    operands = [totals, target, old, split_kernel]
    return pl.pallas_call(
        value_body,
        in_specs=[WHOLE] * 4,
        out_specs=[WHOLE] * 3,
        out_shape=out,
        compiler_params=PARAMS,
        cost_estimate=cost(3 * pairs * split_kernel.size, *operands, *out),
        name="value",
    )(*operands)


def sum_body(pieces_ref, copies_ref):
    total = pieces_ref[0]
    for i in range(1, pieces_ref.shape[0]):
        total = total + pieces_ref[i]
    for i in range(copies_ref.shape[0]):
        copies_ref[i] = total


def summed(pieces, copies):
    out = jax.ShapeDtypeStruct((copies, *pieces.shape[1:]), f32)
    return pl.pallas_call(
        sum_body,
        in_specs=[WHOLE],
        out_specs=WHOLE,
        out_shape=out,
        compiler_params=PARAMS,
        cost_estimate=cost(pieces.size, pieces, out),
        name="sum",
    )(pieces)


def last_body(total_ref, target_ref, old_ref, *refs):
    *terms, right_ref, errors_ref = refs
    error = new_right(total_ref, target_ref, old_ref, right_ref)
    lane = lax.broadcasted_iota(jnp.int32, (error.shape[0], LANES), 1)
    table = jnp.zeros((error.shape[0], LANES), f32)
    for i, term in enumerate([*(t[...] for t in terms), error]):
        table = jnp.where(lane == i, term, table)
    rest = jnp.zeros((LANES - table.shape[0], LANES), f32)
    table = jnp.concatenate([table, rest], axis=0).T[: errors_ref.shape[1]]
    for i in range(errors_ref.shape[0]):
        errors_ref[i] = table


def last_right(totals, target, old, terms, copies):
    pairs = target.shape[0]
    out = [
        jax.ShapeDtypeStruct(target.shape, f32),
        jax.ShapeDtypeStruct((copies, SUBLANES, LANES), f32),
    ]
    operands = [totals, target, old, *terms]
    return pl.pallas_call(
        last_body,
        in_specs=[WHOLE] * len(operands),
        out_specs=[WHOLE] * 2,
        out_shape=out,
        compiler_params=PARAMS,
        cost_estimate=cost(4 * target.size, *operands, *out),
        name="last",
    )(*operands)


def errors_body(count, tables_ref, errors_ref):
    table = tables_ref[0]
    for i in range(1, tables_ref.shape[0]):
        table = table + tables_ref[i]
    errors_ref[...] = table[: errors_ref.shape[0], : errors_ref.shape[1]] / count


def mean_errors(tables, pairs, count):
    out = jax.ShapeDtypeStruct((ITERS, pairs), f32)
    return pl.pallas_call(
        functools.partial(errors_body, count),
        in_specs=[WHOLE],
        out_specs=WHOLE,
        out_shape=out,
        compiler_params=PARAMS,
        cost_estimate=cost(tables.size, tables, out),
        name="errors",
    )(tables)


def exchange(pieces, axis, groups=None):
    return lax.all_to_all(
        pieces, axis, split_axis=0, concat_axis=0, tiled=True, axis_index_groups=groups
    )


def solution(mesh):
    rows, cores = mesh.shape["row"], mesh.shape["rep"]
    far = rows // NEAR
    block = ("col", "rep")
    blocks = mesh.shape["col"] * cores
    lines = ("row", "rep")
    block_group = [[cores - 1] + [i for i in range(blocks) if i != cores - 1]]

    def device(row, core):
        return (row + core * NEAR // cores) % rows * cores + core

    def groups_of(members):
        return [[device(row, core) for row in rows_of] for core in range(cores) for rows_of in members]

    def owner(group, piece):
        return group * NEAR + OWNERS[group][piece]

    near_groups = groups_of([[owner(g, m) for m in range(NEAR)] for g in range(far)])
    far_groups = [
        groups_of(
            [[owner((first + i) % far, m) for i in range(far)] for m, first in enumerate(firsts)]
        )
        for firsts in FAR_FIRST
    ]

    def total_over_rows(pieces, step):
        pieces = summed(exchange(pieces, lines, near_groups), far)
        pieces = summed(exchange(pieces, lines, far_groups[min(step, 1)]), NEAR)
        return exchange(pieces, lines, near_groups)

    def local(kernel, source, target):
        split_kernel, sums = split(kernel, blocks)
        values = exchange(sums, block, block_group)
        right_scale = jnp.ones(target.shape, f32)
        terms = []
        for step in range(ITERS):
            left_scale, pieces = scale_left(values, source, split_kernel)
            totals = total_over_rows(pieces, step)
            if step < ITERS - 1:
                right_scale, term, values = scale_right(
                    totals, target, right_scale, split_kernel, blocks
                )
                values = exchange(values, block, block_group)
                terms.append(term)
        right_scale, tables = last_right(totals, target, right_scale, terms, blocks)
        count = float(blocks * target.shape[1])
        errors = mean_errors(exchange(tables, block, block_group), target.shape[0], count)
        return left_scale, right_scale, errors

    return jax.shard_map(
        local,
        mesh=mesh,
        in_specs=(P(("groups", "row"), block), P("groups", "row"), P("groups", block)),
        out_specs=(P("groups", "row"), P("groups", block), P("groups", None)),
        check_vma=False,
    )
```
